1024 devices in a mesh: dp: 16 (over z, core), seq: 64 (over x, y).
Axes of the slice: x: 8, y: 8, z: 8, core: 2. Of those that a mesh axis runs over, the one named last changes fastest.
Arguments:
- patches: bfloat16 [196608, 1280], P(('dp', 'seq')), may hold values from -6 to 6
- query_key_value: bfloat16 [196608, 3840], P(('dp', 'seq')), may hold values from -100 to 100
- counts: int32 [1024, 4], P(('dp', 'seq')), may hold values from 4 to 48, as said below
- owner_index: int32 [49152, 1], P(('dp', 'seq')), may hold values from 0 to 63; in each aligned block of 48 rows (0 to 47, 48 to 95, ...) at most 2 rows name the same one
- out_weight: bfloat16 [1280, 1280], P(None, 'dp'), may hold values from -0.15625 to 0.15625
- ln_gain: float32 [1280], replicated, may hold values from 0.25 to 1.75
- ln_bias: float32 [1280], replicated, may hold values from -3 to 3
Outputs:
- image_tokens: bfloat16 [131072, 5120], P(('dp', 'seq'))
The draws below stay inside these ranges and needn't reach their ends.
Inputs may be any that keep to these rules, and one draw needn't show every extreme that they name: Every count is a multiple of 4, each device's counts sum to at most 192, and some device's counts sum to exactly 192. `owner_index`: among the merge groups of one device, at most 2 name the same owner.
All inputs are finite; a program needn't handle non-finite values.
Results may differ from the reference program's by a relative error of at most 0.0029.
Values may be sent and summed in bfloat16 or wider, within the bound.
No kernel may reach another device: no remote copies, remote signals or barrier semaphores. Data moves between devices by JAX's collectives and lax.ppermute only.
A program may use at most 32 MiB of HBM per device.

```python
import math
import jax
import jax.numpy as jnp
import numpy as np
from jax import lax

DV = 1280
HEADS = 16
IMGS = 4
PCAP = 192
GROUPS_DEV = 48
CAP = 2
ROWS = 196608
GROUPS = 49152
N_DP = 16
N_SEQ = 64
DEVICES = 1024


def draw_counts(key, part):
    per_image = PCAP // (4 * IMGS)
    lowest = max(1, (3 * per_image + 3) // 4)
    group_counts = jax.random.randint(jax.random.fold_in(key, 11), (DEVICES, IMGS), lowest, per_image + 1)
    full_device = jax.random.randint(jax.random.fold_in(key, 13), (), 0, DEVICES)
    device_ids = jnp.arange(DEVICES, dtype=jnp.int32)
    group_counts = jnp.where(device_ids[:, None] == full_device, per_image, group_counts)
    return (4 * group_counts).astype(jnp.int32)


def draw_query_key_value(key, part):
    base = jnp.clip(jax.random.normal(jax.random.fold_in(key, 21), (ROWS, 3 * DV), jnp.float32), -4.0, 4.0)
    return jnp.clip(base, -100.0, 100.0).astype(jnp.bfloat16)


def steps_of(own_key, extent, pieces, low, top_value):
    level, own = 1.0, jax.random.fold_in(own_key, 6)
    for dim, parts in pieces:
        steps = jnp.exp(jax.random.uniform(jax.random.fold_in(own, dim), (parts,), jnp.float32, low / len(pieces), top_value / len(pieces)))
        level = level * jnp.repeat(steps, extent[dim] // parts).reshape([-1 if axis == dim else 1 for axis in range(len(extent))])
    return level


def shared_out(rng, own, number, rows, number_of, top, most, slope):
    ranking = jax.random.permutation(rng, number_of)
    crowded, common = shares(number_of, rows * top, most, slope, True), shares(number_of, rows * top, most, slope, False)
    places = jnp.arange(number_of)

    def named(sizes, turn):
        used = int((sizes > 0).sum())
        fixed = max(1, used // 4)
        shifted = fixed + (places - fixed + turn * (used - fixed)) % max(1, number_of - fixed)
        return jnp.zeros((number_of,), jnp.int32).at[ranking[jnp.where(places < fixed, places, shifted)]].set(jnp.asarray(sizes, jnp.int32))

    sizes = jnp.where(number % 4 == 0, named(crowded, number // 4), named(common, number - number // 4 - 1))
    mixed = jax.random.permutation(jax.random.fold_in(own, 3), number_of)
    giver, taker = mixed[0:number_of // 2 * 2:2], mixed[1:number_of // 2 * 2:2]
    slack = jnp.minimum(sizes[giver] - 1, most - sizes[taker]) // 2
    slack = jnp.where((giver == ranking[0]) | (taker == ranking[0]) | (sizes[taker] == 0), 0, jnp.maximum(slack, 0))
    shifted = jax.random.randint(jax.random.fold_in(own, 4), (number_of // 2,), 0, 1 << 20) % (slack + 1)
    sizes = sizes.at[giver].add(-shifted).at[taker].add(shifted)
    labels = jnp.searchsorted(jnp.cumsum(sizes), jnp.arange(rows * top), side="right").astype(jnp.int32)
    table = labels.reshape(top, rows).T
    table = table[jax.random.permutation(jax.random.fold_in(own, 1), rows)]
    turn = jax.random.randint(jax.random.fold_in(own, 2), (rows, 1), 0, top)
    return jnp.take_along_axis(table, (jnp.arange(top)[None, :] + turn) % top, axis=1)


def shares(number_of, total, bound, skew, full):
    weights = [(1 << 20) // math.isqrt(rank ** skew) + 1 for rank in range(1, number_of + 1)]
    largest = bound if full else min(bound, max(-(-total // number_of), total * weights[0] // sum(weights)))
    least = 1 if total - largest >= number_of - 1 else 0
    given, surplus = [largest] + [least] * (number_of - 1), total - largest - least * (number_of - 1)
    while surplus > 0:
        free = [i for i in range(1, number_of) if given[i] < largest] or [i for i in range(1, number_of) if given[i] < bound]
        whole, budget = sum([weights[i] for i in free]), surplus
        for i in free:
            more = min(bound - given[i], max(1, budget * weights[i] // whole), surplus)
            given[i] = given[i] + more
            surplus = surplus - more
    return np.array(given)


def scatter_about(key, dims, width, reach, cuts=(), kind=jnp.bfloat16):
    array = width * jax.random.normal(key, dims, jnp.float32)
    if cuts:
        array = array * steps_of(key, dims, cuts, -0.22, 0.18)
    return jnp.clip(array, -reach, reach).astype(kind)


def setup_inputs(seed: int = 0) -> dict:
    seeds = jax.random.split(jax.random.key(seed), 8)
    patches = scatter_about(seeds[0], (ROWS, DV), 1.0, 6.0, ((0, 1024),))
    query_key_value = draw_query_key_value(jax.random.fold_in(seeds[7], 71), 0)
    counts = draw_counts(jax.random.fold_in(seeds[7], 71), 0)
    owner_index_keys = jax.random.split(jax.random.fold_in(seeds[3], 1), GROUPS // GROUPS_DEV)
    owner_index_turns = jax.random.permutation(jax.random.fold_in(seeds[3], 3), GROUPS // GROUPS_DEV)
    owner_index = jax.vmap(lambda own, number: shared_out(jax.random.fold_in(seeds[3], 2), own, number, GROUPS_DEV, N_SEQ, 1, CAP, 1))(owner_index_keys, owner_index_turns).reshape((GROUPS, 1))
    out_weight = scatter_about(seeds[4], (DV, DV), DV ** -0.5, 0.15625, ((1, 16),))
    ln_gain = jnp.clip(1.0 + 0.15 * jax.random.normal(seeds[5], (DV,), jnp.float32), 0.25, 1.75)
    ln_bias = scatter_about(seeds[6], (DV,), 0.5, 3.0, (), jnp.float32)
    return {"patches": patches, "query_key_value": query_key_value, "counts": counts, "owner_index": owner_index, "out_weight": out_weight, "ln_gain": ln_gain, "ln_bias": ln_bias}


def segment_rows(count_row, row_count):
    image_ends = jnp.cumsum(count_row.astype(jnp.int32))
    row_ids = jnp.arange(row_count, dtype=jnp.int32)
    return lax.optimization_barrier(jnp.sum((row_ids[:, None] >= image_ends[None, :]).astype(jnp.int32), axis=1))

def attend(packed, segment_ids, model_width):
    row_count = packed.shape[0]
    head_size = model_width // HEADS
    queries = packed[:, :model_width].astype(jnp.float32).reshape(row_count, HEADS, head_size)
    keys_all = packed[:, model_width:2 * model_width].astype(jnp.float32).reshape(row_count, HEADS, head_size)
    values_all = packed[:, 2 * model_width:].astype(jnp.float32).reshape(row_count, HEADS, head_size)
    scores = jnp.einsum('qhd,khd->hqk', queries, keys_all) * head_size ** (-0.5)
    same_image = segment_ids[:, None] == segment_ids[None, :]
    scores = jnp.where(same_image[None, :, :], scores, -1e+30)
    top_score = lax.optimization_barrier(jnp.max(scores, axis=2, keepdims=True))
    expo = jnp.exp(scores - top_score)
    attn_weights = (expo / lax.optimization_barrier(jnp.sum(expo, axis=2, keepdims=True))).astype(jnp.bfloat16)
    context = jnp.einsum('hqk,khd->qhd', attn_weights.astype(jnp.float32), values_all)
    return context.reshape(row_count, model_width).astype(jnp.bfloat16)

def merge_and_place(hidden, segment_ids, owners, ln_gain, ln_bias, owner_count, capacity):
    row_count, model_width = hidden.shape
    row_mean = lax.optimization_barrier(jnp.mean(hidden, axis=1, keepdims=True))
    centered = hidden - row_mean
    row_var = lax.optimization_barrier(jnp.mean(centered * centered, axis=1, keepdims=True))
    normed = (centered * lax.rsqrt(row_var + 1e-06) * ln_gain[None, :] + ln_bias[None, :]).astype(jnp.bfloat16)
    merged = normed.reshape(row_count // 4, 4 * model_width)
    live_group = segment_ids.reshape(row_count // 4, 4)[:, 0] < IMGS
    group_ids = jnp.arange(row_count // 4, dtype=jnp.int32)
    earlier = (owners[None, :] == owners[:, None]) & (group_ids[None, :] < group_ids[:, None]) & live_group[None, :]
    slot_index = lax.optimization_barrier(jnp.sum(earlier.astype(jnp.int32), axis=1))
    target = owners * capacity + slot_index
    slot_ids = jnp.arange(owner_count * capacity, dtype=jnp.int32)
    onehot_map = ((slot_ids[:, None] == target[None, :]) & live_group[None, :]).astype(jnp.bfloat16)
    return jnp.dot(onehot_map, merged, preferred_element_type=jnp.float32).astype(jnp.bfloat16)

def reference(patches, query_key_value, counts, owner_index, out_weight, ln_gain, ln_bias):
    model_width = patches.shape[1]
    device_count = counts.shape[0]
    patch_blocks = patches.reshape(device_count, PCAP, model_width)
    packed_blocks = query_key_value.reshape(device_count, PCAP, 3 * model_width)
    owner_blocks = owner_index.reshape(device_count, PCAP // 4)

    def one_device(inputs):
        patch_rows, packed, count_row, owners = inputs
        segment_ids = segment_rows(count_row, PCAP)
        context = attend(packed, segment_ids, model_width)
        hidden = patch_rows.astype(jnp.float32) + jnp.dot(context, out_weight, preferred_element_type=jnp.float32)
        return merge_and_place(hidden, segment_ids, owners, ln_gain, ln_bias, N_SEQ, CAP)
    outgoing = lax.map(one_device, (patch_blocks, packed_blocks, counts, owner_blocks))
    outgoing = outgoing.reshape(N_DP, N_SEQ, N_SEQ, CAP, 4 * model_width)
    outgoing = jnp.transpose(outgoing, (0, 2, 1, 3, 4))
    return outgoing.reshape(device_count * N_SEQ * CAP, 4 * model_width)
```

```python
import functools

import jax
import jax.numpy as jnp
from jax import lax
from jax.experimental import pallas as pl
from jax.experimental.pallas import tpu as pltpu
from jax.sharding import PartitionSpec as P


HEADS = 16
IMGS = 4
DEAD = -1000
VMEM = pl.BlockSpec(memory_space=pltpu.VMEM)
SMEM = pl.BlockSpec(memory_space=pltpu.SMEM)
HBM = pl.BlockSpec(memory_space=pltpu.HBM)
F32 = jnp.float32
BF16 = jnp.bfloat16


def iota(shape, dim):
    return lax.broadcasted_iota(jnp.int32, shape, dim)


def pick(hits, values):
    return lax.dot_general(
        jnp.where(hits, 1.0, 0.0).astype(BF16), values, (((1,), (0,)), ((), ())), preferred_element_type=F32
    )


def call(kernel, out_shape, operands, flops, scratch=(), smem=0, limit=8, out_specs=VMEM):
    return pl.pallas_call(
        kernel,
        out_shape=out_shape,
        in_specs=[SMEM] * smem + [VMEM] * (len(operands) - smem),
        out_specs=out_specs,
        scratch_shapes=list(scratch),
        compiler_params=pltpu.CompilerParams(vmem_limit_bytes=limit * 1024 * 1024),
        cost_estimate=pl.CostEstimate(flops=flops, bytes_accessed=1 << 20, transcendentals=0),
    )(*operands)


def image_ends(counts_ref):
    ends, end = [], 0
    for image in range(IMGS):
        end = end + counts_ref[0, image]
        ends.append(end)
    return ends


def row_slots(ends, owner_row, owner_col):
    rows = owner_row.shape[1]
    lane, sub = iota((1, rows), 1), iota((rows, 1), 0)
    first = lane - (lane & 3)
    earlier = (owner_col == owner_row) & (sub < first) & ((sub & 3) == 0) & (sub < ends[-1])
    slot = jnp.sum(jnp.where(earlier, 1.0, 0.0), axis=0, keepdims=True)
    return slot, first < ends[-1], lane & 3


def front_kernel(
    counts_ref, owner_row_ref, owner_col_ref, packed_ref, patch_ref, context_out, send_ref, context_ref, done
):
    rows, width = patch_ref.shape
    head_size = width // HEADS
    ends = image_ends(counts_ref)
    lane, sub = iota((1, rows), 1), iota((rows, 1), 0)
    segment_row = sum((lane >= end).astype(jnp.int32) for end in ends)
    segment_col = sum((sub >= end).astype(jnp.int32) for end in ends)
    same_image = segment_col == segment_row
    for head in range(HEADS):
        low = head * head_size
        start = min(low // 128 * 128, width - 256)
        column = iota((1, 256), 1) + start
        mine = (column >= low) & (column < low + head_size)
        queries = packed_ref[:, start : start + 256]
        queries = jnp.where(mine, queries, jnp.zeros_like(queries))
        keys = packed_ref[:, width + start : width + start + 256]
        scores = lax.dot_general(
            queries, keys, (((1,), (1,)), ((), ())), preferred_element_type=F32
        ) * head_size ** (-0.5)
        scores = jnp.where(same_image, scores, -1e30)
        expo = jnp.exp(scores - jnp.max(scores, axis=1, keepdims=True))
        weights = (expo / jnp.sum(expo, axis=1, keepdims=True)).astype(BF16)
        values = packed_ref[:, 2 * width + start : 2 * width + start + 256]
        mixed = jnp.dot(weights, values, preferred_element_type=F32).astype(BF16)
        context_ref[:, start : start + 256] = jnp.where(mine, mixed, context_ref[:, start : start + 256])
    leave = pltpu.make_async_copy(context_ref, context_out, done)
    leave.start()
    slot, live, part = row_slots(ends, owner_row_ref[...], owner_col_ref[...])
    key = jnp.where(live & (slot == 0.0), owner_row_ref[...] * 8 + part, DEAD)
    line = iota((send_ref.shape[0], 1), 0)
    hits = key == line
    held = jnp.sum(jnp.where(hits, 1.0, 0.0), axis=1, keepdims=True)
    marker = jnp.where((held == 0.0) & ((line & 7) < 4), 64.0, 0.0)
    sent = pick(hits, patch_ref[...]) + pick(key == line - 4, context_ref[...]) + marker
    send_ref[...] = sent.astype(BF16)
    leave.wait()


def norm(hidden, gain, bias):
    gain, bias = gain[None, :], bias[None, :]
    inverse = 1.0 / hidden.shape[1]
    centered = hidden - jnp.sum(hidden, axis=1, keepdims=True) * inverse
    row_var = jnp.sum(centered * centered, axis=1, keepdims=True) * inverse
    return centered * lax.rsqrt(row_var + 1e-06) * gain + bias


def project(context, weight):
    return lax.dot_general(context, weight, (((1,), (1,)), ((), ())), preferred_element_type=F32)


def late_kernel(nz, splits, counts_ref, *refs):
    blocks, refs = refs[:nz], refs[nz:]
    halves, refs = refs[: len(splits)], refs[len(splits) :]
    owner_row_ref, owner_col_ref, context_ref, patch_ref, gain_ref, bias_ref = refs[:6]
    weight_out, send_ref, weight_ref, done = refs[6:]
    block_width = blocks[0].shape[0]
    me = lax.axis_index("dp")
    z, c = lax.shift_right_logical(me, 1), lax.bitwise_and(me, 1)

    def put(j, core, value):
        owner = lax.rem(z + j, nz) * 2 + core
        weight_ref[pl.ds(pl.multiple_of(owner * block_width, 16), block_width), :] = value

    for j in range(nz):
        put(j, c, blocks[j][...])
    for part, ref in zip(splits, halves):
        for i, j in enumerate(part):
            put(j, 1 - c, ref[i])
    leave = pltpu.make_async_copy(weight_ref, weight_out, done)
    leave.start()
    hidden = patch_ref[...].astype(F32) + project(context_ref[...], weight_ref[...])
    normed = norm(hidden, gain_ref[...], bias_ref[...]).astype(BF16)
    slot, live, part = row_slots(image_ends(counts_ref), owner_row_ref[...], owner_col_ref[...])
    key = jnp.where(live & (slot == 1.0), owner_row_ref[...] * 8 + 2 * part, DEAD)
    line = iota((send_ref.shape[0], 1), 0)
    half = send_ref.shape[1]
    sent = pick(key == line, normed[:, :half]) + pick(key == line - 1, normed[:, half:])
    send_ref[...] = sent.astype(BF16)
    leave.wait()


def early_kernel(received_ref, weight_ref, gain_ref, bias_ref, normed_ref):
    lines = received_ref.shape[0]
    owners = lines // 8
    row = iota((4 * owners, 1), 0)
    shift = owners.bit_length() - 1
    line = (row & (owners - 1)) * 8 + (row >> shift)
    column = iota((1, lines), 1)
    patches = pick(column == line, received_ref[...])
    context = pick(column == line + 4, received_ref[...]).astype(BF16)
    hidden = patches + project(context, weight_ref[...])
    normed = norm(hidden, gain_ref[...], bias_ref[...])
    normed_ref[...] = jnp.where(patches[:, :1] > 32.0, 0.0, normed).astype(BF16)


def join_kernel(normed_ref, received_ref, out_ref):
    lines, half = received_ref.shape
    owners = lines // 8
    row = iota((2 * owners, 1), 0)
    even = row == 2 * iota((1, owners), 1)
    column = iota((1, lines), 1)
    odd = (row & 1) == 1
    for part in range(4):
        for side in range(2):
            first = pick(even, normed_ref[part * owners : (part + 1) * owners, side * half : (side + 1) * half])
            hits = (column == 4 * (row - 1) + 2 * part + side) & odd
            start = (2 * part + side) * half
            out_ref[:, start : start + half] = (first + pick(hits, received_ref[...])).astype(BF16)


def pack_kernel(*refs):
    for i, ref in enumerate(refs[:-1]):
        refs[-1][i] = ref[...]


def pack(blocks):
    shape = jax.ShapeDtypeStruct((len(blocks), *blocks[0].shape), blocks[0].dtype)
    return call(pack_kernel, shape, blocks, 1 << 20, limit=1)


def ring_gather(shard):
    n_dp = lax.axis_size("dp")
    nz = n_dp // 2
    up = [(2 * z + c, 2 * ((z + 1) % nz) + c) for z in range(nz) for c in range(2)]
    down = [(2 * z + c, 2 * ((z - 1) % nz) + c) for z in range(nz) for c in range(2)]
    swap = [(d, d ^ 1) for d in range(n_dp)]
    blocks = [None] * nz
    blocks[0] = shard
    from_below, from_above = shard, shard
    for step in range(1, nz // 2 + 1):
        from_below = lax.ppermute(from_below, "dp", up)
        blocks[(-step) % nz] = from_below
        if step < nz - step:
            from_above = lax.ppermute(from_above, "dp", down)
            blocks[step] = from_above
    order = sorted(range(nz), key=lambda j: min(j, nz - j))
    splits = [s for s in (order[: nz // 2 + 1], order[nz // 2 + 1 :]) if s]
    halves = [lax.ppermute(pack([blocks[j] for j in part]), "dp", swap) for part in splits]
    return blocks, splits, halves


def step(patches, query_key_value, counts, owner_index, out_weight, ln_gain, ln_bias):
    rows, width = patches.shape
    owners = lax.axis_size("seq")
    nz = lax.axis_size("dp") // 2
    owner_col = jnp.repeat(owner_index, 4, axis=0)
    owner_row = owner_col.reshape(1, rows)

    blocks, splits, halves = ring_gather(out_weight.T)
    context, send = call(
      front_kernel,
      (pltpu.HBM((rows, width), BF16), jax.ShapeDtypeStruct((8 * owners, width), BF16)),
      [counts, owner_row, owner_col, query_key_value, patches],
      1 << 31,
      scratch=[pltpu.VMEM((rows, width), BF16), pltpu.SemaphoreType.DMA],
      smem=1,
      out_specs=(HBM, VMEM),
    )
    received = lax.all_to_all(send, "seq", split_axis=0, concat_axis=0, tiled=True)
    weight, late_send = call(
        functools.partial(late_kernel, nz, splits),
        (pltpu.HBM((width, width), BF16), jax.ShapeDtypeStruct((8 * owners, width // 2), BF16)),
        [counts, *blocks, *halves, owner_row, owner_col, context, patches, ln_gain, ln_bias],
        2 * rows * width * width,
        scratch=[pltpu.VMEM((width, width), BF16), pltpu.SemaphoreType.DMA],
        smem=1,
        out_specs=(HBM, VMEM),
    )
    late_received = lax.all_to_all(late_send, "seq", split_axis=0, concat_axis=0, tiled=True)
    normed = call(
        early_kernel,
        jax.ShapeDtypeStruct((4 * owners, width), BF16),
        [received, weight, ln_gain, ln_bias],
        8 * owners * width * width,
    )
    return call(join_kernel, jax.ShapeDtypeStruct((2 * owners, 4 * width), BF16), [normed, late_received], 1 << 29)


def solution(mesh):
    placed = (
        P(("dp", "seq"), None),
        P(("dp", "seq"), None),
        P(("dp", "seq"), None),
        P(("dp", "seq"), None),
        P(None, "dp"),
        P(),
        P(),
    )
    return jax.shard_map(step, mesh=mesh, in_specs=placed, out_specs=P(("dp", "seq"), None), check_vma=False)
```

```python
import functools

import jax
import jax.numpy as jnp
from jax import lax
from jax.experimental import pallas as pl
from jax.experimental.pallas import tpu as pltpu
from jax.sharding import PartitionSpec as P


HEADS = 16
IMGS = 4
DEAD = -1000
VMEM = pl.BlockSpec(memory_space=pltpu.VMEM)
SMEM = pl.BlockSpec(memory_space=pltpu.SMEM)
HBM = pl.BlockSpec(memory_space=pltpu.HBM)
F32 = jnp.float32
BF16 = jnp.bfloat16


def iota(shape, dim):
    return lax.broadcasted_iota(jnp.int32, shape, dim)


def pick(hits, values):
    return lax.dot_general(
        jnp.where(hits, 1.0, 0.0).astype(BF16), values, (((1,), (0,)), ((), ())), preferred_element_type=F32
    )


def call(kernel, out_shape, operands, flops, scratch=(), smem=0, limit=8, out_specs=VMEM, in_specs=None):
    return pl.pallas_call(
        kernel,
        out_shape=out_shape,
        in_specs=in_specs or [SMEM] * smem + [VMEM] * (len(operands) - smem),
        out_specs=out_specs,
        scratch_shapes=list(scratch),
        compiler_params=pltpu.CompilerParams(vmem_limit_bytes=limit * 1024 * 1024),
        cost_estimate=pl.CostEstimate(flops=flops, bytes_accessed=1 << 20, transcendentals=0),
    )(*operands)


def image_ends(counts_ref):
    ends, end = [], 0
    for image in range(IMGS):
        end = end + counts_ref[0, image]
        ends.append(end)
    return ends


def row_slots(ends, owner_ref, rows):
    groups = owner_ref.shape[1]
    lane, sub = iota((1, rows), 1), iota((rows, 1), 0)
    owners = jnp.broadcast_to(owner_ref[...], (8, groups)).astype(F32).astype(BF16)
    spread = jnp.where((iota((1, rows), 1) >> 2) == iota((groups, 1), 0), 1.0, 0.0).astype(BF16)
    owner_row = jnp.dot(owners, spread, preferred_element_type=F32)[0:1, :]
    owner_col = jnp.sum(jnp.where(sub == lane, owner_row, 0.0), axis=1, keepdims=True)
    first = lane - (lane & 3)
    earlier = (owner_col == owner_row) & (sub < first) & ((sub & 3) == 0) & (sub < ends[-1])
    slot = jnp.sum(jnp.where(earlier, 1.0, 0.0), axis=0, keepdims=True)
    return owner_row.astype(jnp.int32), slot, first < ends[-1], lane & 3


def front_kernel(
    counts_in, owner_in, packed_in, patch_in, context_out, send_ref,
    counts_ref, owner_ref, packed_ref, patch_ref, context_ref, done
):
    rows, width = patch_ref.shape
    head_size = width // HEADS
    pairs = ((counts_in, counts_ref), (packed_in, packed_ref), (owner_in, owner_ref), (patch_in, patch_ref))
    fetches = [pltpu.make_async_copy(src, dst, done.at[i]) for i, (src, dst) in enumerate(pairs)]
    for fetch in fetches:
        fetch.start()
    context_ref[...] = jnp.zeros_like(context_ref)
    fetches[0].wait()
    fetches[1].wait()
    ends = image_ends(counts_ref)
    lane, sub = iota((1, rows), 1), iota((rows, 1), 0)
    segment_row = sum((lane >= end).astype(jnp.int32) for end in ends)
    segment_col = sum((sub >= end).astype(jnp.int32) for end in ends)
    same_image = segment_col == segment_row
    for head in range(HEADS):
        low = head * head_size
        start = min(low // 128 * 128, width - 256)
        column = iota((1, 256), 1) + start
        mine = (column >= low) & (column < low + head_size)
        queries = packed_ref[:, start : start + 256]
        queries = jnp.where(mine, queries, jnp.zeros_like(queries))
        keys = packed_ref[:, width + start : width + start + 256]
        scores = lax.dot_general(
            queries, keys, (((1,), (1,)), ((), ())), preferred_element_type=F32
        ) * head_size ** (-0.5)
        scores = jnp.where(same_image, scores, -1e30)
        expo = jnp.exp(scores - jnp.max(scores, axis=1, keepdims=True))
        weights = (expo / jnp.sum(expo, axis=1, keepdims=True)).astype(BF16)
        values = packed_ref[:, 2 * width + start : 2 * width + start + 256]
        mixed = jnp.dot(weights, values, preferred_element_type=F32).astype(BF16)
        context_ref[:, start : start + 256] = jnp.where(mine, mixed, context_ref[:, start : start + 256])
    leave = pltpu.make_async_copy(context_ref, context_out, done.at[4])
    leave.start()
    fetches[2].wait()
    fetches[3].wait()
    owner_row, slot, live, part = row_slots(ends, owner_ref, rows)
    key = jnp.where(live & (slot == 0.0), owner_row * 8 + part, DEAD)
    line = iota((send_ref.shape[0], 1), 0)
    hits = key == line
    held = jnp.sum(jnp.where(hits, 1.0, 0.0), axis=1, keepdims=True)
    marker = jnp.where((held == 0.0) & ((line & 7) < 4), 64.0, 0.0)
    sent = pick(hits, patch_ref[...]) + pick(key == line - 4, context_ref[...]) + marker
    send_ref[...] = sent.astype(BF16)
    leave.wait()


def norm(hidden, gain, bias):
    gain, bias = gain[None, :], bias[None, :]
    inverse = 1.0 / hidden.shape[1]
    centered = hidden - jnp.sum(hidden, axis=1, keepdims=True) * inverse
    row_var = jnp.sum(centered * centered, axis=1, keepdims=True) * inverse
    return centered * lax.rsqrt(row_var + 1e-06) * gain + bias


def project(context, weight):
    return lax.dot_general(context, weight, (((1,), (1,)), ((), ())), preferred_element_type=F32)


def late_kernel(nz, splits, counts_ref, *refs):
    blocks, refs = refs[:nz], refs[nz:]
    halves, refs = refs[: len(splits)], refs[len(splits) :]
    owner_ref, context_ref, patch_ref, gain_ref, bias_ref = refs[:5]
    weight_out, send_ref, weight_ref, done = refs[5:]
    block_width = blocks[0].shape[0]
    me = lax.axis_index("dp")
    z, c = lax.shift_right_logical(me, 1), lax.bitwise_and(me, 1)
    pieces = [(j, c, blocks[j]) for j in range(nz)]
    for part, ref in zip(splits, halves):
        pieces += [(j, 1 - c, ref.at[i]) for i, j in enumerate(part)]
    leaves, places = [], []
    for i, (j, core, ref) in enumerate(pieces):
        owner = lax.rem(z + j * (1 - 2 * core) + nz, nz) * 2 + core
        places.append(pl.ds(pl.multiple_of(owner * block_width, 16), block_width))
        leaves.append(pltpu.make_async_copy(ref, weight_out.at[places[i], :], done.at[i]))
        leaves[i].start()
    for place, (_, _, ref) in zip(places, pieces):
        weight_ref[place, :] = ref[...]
    hidden = patch_ref[...].astype(F32) + project(context_ref[...], weight_ref[...])
    normed = norm(hidden, gain_ref[...], bias_ref[...]).astype(BF16)
    owner_row, slot, live, part = row_slots(image_ends(counts_ref), owner_ref, patch_ref.shape[0])
    key = jnp.where(live & (slot == 1.0), owner_row * 8 + 2 * part, DEAD)
    line = iota((send_ref.shape[0], 1), 0)
    half = send_ref.shape[1]
    sent = pick(key == line, normed[:, :half]) + pick(key == line - 1, normed[:, half:])
    send_ref[...] = sent.astype(BF16)
    for leave in leaves:
        leave.wait()


def early_kernel(received_ref, weight_ref, gain_ref, bias_ref, out_ref):
    lines, width = received_ref.shape
    owners = lines // 8
    row = iota((4 * owners, 1), 0)
    place = (row & (owners - 1)) * 8 + (row >> (owners.bit_length() - 1))
    column = iota((1, lines), 1)
    patches = pick(column == place, received_ref[...])
    context = pick(column == place + 4, received_ref[...]).astype(BF16)
    normed = norm(patches + project(context, weight_ref[...]), gain_ref[...], bias_ref[...])
    normed = jnp.where(patches[:, :1] > 32.0, 0.0, normed).astype(BF16)
    even = iota((2 * owners, 1), 0) == 2 * iota((1, owners), 1)
    for part in range(4):
        first = pick(even, normed[part * owners : (part + 1) * owners, :])
        out_ref[:, part * width : (part + 1) * width] = first.astype(BF16)


def join_kernel(first_ref, received_ref, out_ref, joined_ref, done):
    lines, half = received_ref.shape
    slots = lines // 4
    row = iota((8 * slots, 1), 0)
    slot, chunk = row & (slots - 1), row >> (slots.bit_length() - 1)
    hits = (iota((1, lines), 1) == 4 * (slot - 1) + chunk) & ((slot & 1) == 1)
    second = pick(hits, received_ref[...]).astype(BF16)
    leaves = []
    for i in range(8):
        columns = slice(i * half, (i + 1) * half)
        joined_ref[:, columns] = first_ref[:, columns] + second[i * slots : (i + 1) * slots]
        leave = pltpu.make_async_copy(joined_ref.at[:, columns], out_ref.at[:, columns], done.at[i])
        leave.start()
        leaves.append(leave)
    for leave in leaves:
        leave.wait()


def pack_kernel(*refs):
    for i, ref in enumerate(refs[:-1]):
        refs[-1][i] = ref[...]


def pack(blocks):
    shape = jax.ShapeDtypeStruct((len(blocks), *blocks[0].shape), blocks[0].dtype)
    return call(pack_kernel, shape, blocks, 1 << 20, limit=1)


def ring_gather(shard):
    n_dp = lax.axis_size("dp")
    nz = n_dp // 2
    up = [(2 * z + c, 2 * ((z + 1 - 2 * c) % nz) + c) for z in range(nz) for c in range(2)]
    down = [(there, here) for here, there in up]
    swap = [(d, d ^ 1) for d in range(n_dp)]
    blocks = [None] * nz
    blocks[0] = shard
    from_below, from_above = shard, shard
    for step in range(1, nz // 2 + 1):
        from_below = lax.ppermute(from_below, "dp", up)
        blocks[(-step) % nz] = from_below
        if step < nz - step:
            from_above = lax.ppermute(from_above, "dp", down)
            blocks[step] = from_above
    order = sorted(range(nz), key=lambda j: min(j, nz - j))
    splits = [s for s in (order[: nz // 2 + 1], order[nz // 2 + 1 :]) if s]
    halves = [lax.ppermute(pack([blocks[j] for j in part]), "dp", swap) for part in splits]
    return blocks, splits, halves


def step(patches, query_key_value, counts, owner_index, out_weight, ln_gain, ln_bias):
    rows, width = patches.shape
    owners = lax.axis_size("seq")
    nz = lax.axis_size("dp") // 2
    owner_lanes = owner_index.reshape(1, rows // 4)
    lines = 8 * owners

    blocks, splits, halves = ring_gather(out_weight.T)
    context, send = call(
        front_kernel,
        (pltpu.HBM((rows, width), BF16), jax.ShapeDtypeStruct((lines, width), BF16)),
        [pltpu.with_memory_space_constraint(x, pltpu.HBM) for x in (counts, owner_lanes, query_key_value, patches)],
        1 << 31,
        scratch=[
            pltpu.SMEM(counts.shape, jnp.int32),
            pltpu.VMEM(owner_lanes.shape, jnp.int32),
            pltpu.VMEM((rows, 3 * width), BF16),
            pltpu.VMEM((rows, width), BF16),
            pltpu.VMEM((rows, width), BF16),
            pltpu.SemaphoreType.DMA((5,)),
        ],
        out_specs=(HBM, VMEM),
        in_specs=[HBM] * 4,
        limit=16,
    )
    received = lax.all_to_all(send, "seq", split_axis=0, concat_axis=0, tiled=True)
    weight, late_send = call(
        functools.partial(late_kernel, nz, splits),
        (pltpu.HBM((width, width), BF16), jax.ShapeDtypeStruct((lines, width // 2), BF16)),
        [counts, *blocks, *halves, owner_lanes, context, patches, ln_gain, ln_bias],
        2 * rows * width * width,
        scratch=[pltpu.VMEM((width, width), BF16), pltpu.SemaphoreType.DMA((2 * nz,))],
        smem=1,
        out_specs=(HBM, VMEM),
    )
    late_received = lax.all_to_all(late_send, "seq", split_axis=0, concat_axis=0, tiled=True)
    shape = jax.ShapeDtypeStruct((2 * owners, 4 * width), BF16)
    first = call(early_kernel, shape, [received, weight, ln_gain, ln_bias], 1 << 31)
    return call(
        join_kernel,
        pltpu.HBM(shape.shape, BF16),
        [first, late_received],
        1 << 29,
        scratch=[pltpu.VMEM(shape.shape, BF16), pltpu.SemaphoreType.DMA((8,))],
        out_specs=HBM,
    )


def solution(mesh):
    placed = (
        P(("dp", "seq"), None),
        P(("dp", "seq"), None),
        P(("dp", "seq"), None),
        P(("dp", "seq"), None),
        P(None, "dp"),
        P(),
        P(),
    )
    return jax.shard_map(step, mesh=mesh, in_specs=placed, out_specs=P(("dp", "seq"), None), check_vma=False)
```

```python
import functools

import jax
import jax.numpy as jnp
from jax import lax
from jax.experimental import pallas as pl
from jax.experimental.pallas import tpu as pltpu
from jax.sharding import PartitionSpec as P

HEADS = 16
IMGS = 4
DEAD = -1000
VMEM = pl.BlockSpec(memory_space=pltpu.VMEM)
SMEM = pl.BlockSpec(memory_space=pltpu.SMEM)
HBM = pl.BlockSpec(memory_space=pltpu.HBM)
F32 = jnp.float32
BF16 = jnp.bfloat16


def iota(shape, dim):
    return lax.broadcasted_iota(jnp.int32, shape, dim)


def pick(hits, values):
    return lax.dot_general(
        jnp.where(hits, 1.0, 0.0).astype(BF16), values, (((1,), (0,)), ((), ())), preferred_element_type=F32
    )


def call(kernel, out_shape, operands, flops, scratch=(), smem=0, limit=8, out_specs=VMEM, in_specs=None):
    return pl.pallas_call(
        kernel,
        out_shape=out_shape,
        in_specs=in_specs or [SMEM] * smem + [VMEM] * (len(operands) - smem),
        out_specs=out_specs,
        scratch_shapes=list(scratch),
        compiler_params=pltpu.CompilerParams(vmem_limit_bytes=limit * 1024 * 1024),
        cost_estimate=pl.CostEstimate(flops=flops, bytes_accessed=1 << 20, transcendentals=0),
    )(*operands)


def image_ends(counts_ref):
    ends, end = [], 0
    for image in range(IMGS):
        end = end + counts_ref[0, image]
        ends.append(end)
    return ends


def row_slots(ends, owner_ref, rows):
    groups = owner_ref.shape[1]
    lane, sub = iota((1, rows), 1), iota((rows, 1), 0)
    owners = jnp.broadcast_to(owner_ref[...], (8, groups)).astype(F32).astype(BF16)
    spread = jnp.where((iota((1, rows), 1) >> 2) == iota((groups, 1), 0), 1.0, 0.0).astype(BF16)
    owner_row = jnp.dot(owners, spread, preferred_element_type=F32)[0:1, :]
    owner_col = jnp.sum(jnp.where(sub == lane, owner_row, 0.0), axis=1, keepdims=True)
    first = lane - (lane & 3)
    earlier = (owner_col == owner_row) & (sub < first) & ((sub & 3) == 0) & (sub < ends[-1])
    slot = jnp.sum(jnp.where(earlier, 1.0, 0.0), axis=0, keepdims=True)
    return owner_row.astype(jnp.int32), slot, first < ends[-1], lane & 3


def front_kernel(
    counts_in, owner_in, packed_in, patch_in, send_out,
    counts_ref, owner_ref, packed_ref, patch_ref, context_ref, send_ref, done, left
):
    rows, width = patch_ref.shape
    head_size = width // HEADS
    pairs = ((counts_in, counts_ref), (owner_in, owner_ref), (patch_in, patch_ref), (packed_in, packed_ref))
    fetches = [pltpu.make_async_copy(src, dst, done.at[i]) for i, (src, dst) in enumerate(pairs)]
    for fetch in fetches:
        fetch.start()
    context_ref[...] = jnp.zeros_like(context_ref)
    for fetch in fetches[:3]:
        fetch.wait()
    ends = image_ends(counts_ref)
    owner_row, slot, live, part = row_slots(ends, owner_ref, rows)
    key = jnp.where(live, owner_row * 8 + slot.astype(jnp.int32) * 4 + part, DEAD)
    lines = send_ref.shape[0]
    hits = key == iota((lines, 1), 0)
    held = jnp.sum(jnp.where(hits, 1.0, 0.0), axis=1, keepdims=True)
    marker = jnp.where(held == 0.0, 64.0, 0.0)
    send_ref[:, :width] = (pick(hits, patch_ref[...]) + marker).astype(BF16)
    leaves = [pltpu.make_async_copy(send_ref.at[:, :width], send_out.at[:, :width], left.at[4])]
    leaves[0].start()
    fetches[3].wait()
    lane, sub = iota((1, rows), 1), iota((rows, 1), 0)
    segment_row = sum((lane >= end).astype(jnp.int32) for end in ends)
    segment_col = sum((sub >= end).astype(jnp.int32) for end in ends)
    same_image = segment_col == segment_row
    for head in range(HEADS):
        low = head * head_size
        start = min(low // 128 * 128, width - 256)
        column = iota((1, 256), 1) + start
        mine = (column >= low) & (column < low + head_size)
        queries = packed_ref[:, start : start + 256]
        queries = jnp.where(mine, queries, jnp.zeros_like(queries))
        keys = packed_ref[:, width + start : width + start + 256]
        scores = lax.dot_general(
            queries, keys, (((1,), (1,)), ((), ())), preferred_element_type=F32
        ) * head_size ** (-0.5)
        scores = jnp.where(same_image, scores, -1e30)
        expo = jnp.exp(scores - jnp.max(scores, axis=1, keepdims=True))
        weights = (expo / jnp.sum(expo, axis=1, keepdims=True)).astype(BF16)
        values = packed_ref[:, 2 * width + start : 2 * width + start + 256]
        mixed = jnp.dot(weights, values, preferred_element_type=F32).astype(BF16)
        context_ref[:, start : start + 256] = jnp.where(mine, mixed, context_ref[:, start : start + 256])
    for i in range(4):
        place = slice(i * lines // 4, (i + 1) * lines // 4)
        wanted = iota((lines // 4, 1), 0) + i * lines // 4
        send_ref[place, width:] = pick(key == wanted, context_ref[...]).astype(BF16)
        leave = pltpu.make_async_copy(send_ref.at[place, width:], send_out.at[place, width:], left.at[i])
        leave.start()
        leaves.append(leave)
    for leave in leaves:
        leave.wait()


def norm(hidden, gain, bias):
    gain, bias = gain[None, :], bias[None, :]
    inverse = 1.0 / hidden.shape[1]
    centered = hidden - jnp.sum(hidden, axis=1, keepdims=True) * inverse
    row_var = jnp.sum(centered * centered, axis=1, keepdims=True) * inverse
    return centered * lax.rsqrt(row_var + 1e-06) * gain + bias


def project(context, weight):
    return lax.dot_general(context, weight, (((1,), (1,)), ((), ())), preferred_element_type=F32)


def gather_kernel(nz, splits, *refs):
    blocks, halves, (weight_out, done) = refs[:nz], refs[nz : nz + len(splits)], refs[nz + len(splits) :]
    block_width = blocks[0].shape[0]
    me = lax.axis_index("dp")
    z, c = lax.shift_right_logical(me, 1), lax.bitwise_and(me, 1)
    pieces = [(j, c, blocks[j]) for j in range(nz)]
    for part, ref in zip(splits, halves):
        pieces += [(j, 1 - c, ref.at[i]) for i, j in enumerate(part)]
    leaves = []
    for i, (j, core, ref) in enumerate(pieces):
        owner = lax.rem(z + j * (1 - 2 * core) + nz, nz) * 2 + core
        place = pl.ds(pl.multiple_of(owner * block_width, 16), block_width)
        leaves.append(pltpu.make_async_copy(ref, weight_out.at[place, :], done.at[i]))
        leaves[i].start()
    for leave in leaves:
        leave.wait()


def finish_kernel(weight_in, received_ref, gain_ref, bias_ref, out_ref, weight_ref, hidden_ref, joined_ref, done):
    lines, width = hidden_ref.shape
    step = 256
    fetches = []
    for i in range(width // step):
        part = slice(i * step, (i + 1) * step)
        fetches.append(pltpu.make_async_copy(weight_in.at[part, :], weight_ref.at[part, :], done.at[i]))
        fetches[i].start()
    for i, fetch in enumerate(fetches):
        fetch.wait()
        part = slice(i * step, (i + 1) * step)
        patches = received_ref[:, part].astype(F32)
        hidden_ref[:, part] = patches + project(received_ref[:, width:], weight_ref[part, :])
    leaves = []
    chunk = min(256, lines)
    slots = chunk // 4
    row = iota((chunk, 1), 0)
    wanted = (row & (slots - 1)) * 4 + (row >> (slots.bit_length() - 1))
    hits = iota((1, chunk), 1) == wanted
    for i in range(lines // chunk):
        part = slice(i * chunk, (i + 1) * chunk)
        normed = norm(hidden_ref[part, :], gain_ref[...], bias_ref[...])
        normed = jnp.where(received_ref[part, :1].astype(F32) > 32.0, 0.0, normed).astype(BF16)
        joined = pick(hits, normed).astype(BF16)
        place = slice(i * slots, (i + 1) * slots)
        for k in range(4):
            joined_ref[place, k * width : (k + 1) * width] = joined[k * slots : (k + 1) * slots]
        leave = pltpu.make_async_copy(joined_ref.at[place, :], out_ref.at[place, :], done.at[8 + i])
        leave.start()
        leaves.append(leave)
    for leave in leaves:
        leave.wait()


def pack_kernel(*refs):
    for i, ref in enumerate(refs[:-1]):
        refs[-1][i] = ref[...]


def pack(blocks):
    shape = jax.ShapeDtypeStruct((len(blocks), *blocks[0].shape), blocks[0].dtype)
    return call(pack_kernel, shape, blocks, 1 << 20, limit=1)


def ring_gather(shard):
    n_dp = lax.axis_size("dp")
    nz = n_dp // 2
    up = [(2 * z + c, 2 * ((z + 1 - 2 * c) % nz) + c) for z in range(nz) for c in range(2)]
    down = [(there, here) for here, there in up]
    swap = [(d, d ^ 1) for d in range(n_dp)]
    blocks = [None] * nz
    blocks[0] = shard
    from_below, from_above = shard, shard
    for step in range(1, nz // 2 + 1):
        from_below = lax.ppermute(from_below, "dp", up)
        blocks[(-step) % nz] = from_below
        if step < nz - step:
            from_above = lax.ppermute(from_above, "dp", down)
            blocks[step] = from_above
    order = sorted(range(nz), key=lambda j: min(j, nz - j))
    splits = [s for s in (order[: nz // 2 + 1], order[nz // 2 + 1 :]) if s]
    halves = [lax.ppermute(pack([blocks[j] for j in part]), "dp", swap) for part in splits]
    return blocks, splits, halves


def step(patches, query_key_value, counts, owner_index, out_weight, ln_gain, ln_bias):
    rows, width = patches.shape
    owners = lax.axis_size("seq")
    nz = lax.axis_size("dp") // 2
    owner_lanes = owner_index.reshape(1, rows // 4)
    lines = 8 * owners

    blocks, splits, halves = ring_gather(out_weight.T)
    send = call(
        front_kernel,
        pltpu.HBM((lines, 2 * width), BF16),
        [pltpu.with_memory_space_constraint(x, pltpu.HBM) for x in (counts, owner_lanes, query_key_value, patches)],
        1 << 31,
        scratch=[
            pltpu.SMEM(counts.shape, jnp.int32),
            pltpu.VMEM(owner_lanes.shape, jnp.int32),
            pltpu.VMEM((rows, 3 * width), BF16),
            pltpu.VMEM((rows, width), BF16),
            pltpu.VMEM((rows, width), BF16),
            pltpu.VMEM((lines, 2 * width), BF16),
            pltpu.SemaphoreType.DMA((4,)),
            pltpu.SemaphoreType.DMA((5,)),
        ],
        in_specs=[HBM] * 4,
        out_specs=HBM,
        limit=16,
    )
    received = lax.all_to_all(send, "seq", split_axis=0, concat_axis=0, tiled=True)
    weight = call(
        functools.partial(gather_kernel, nz, splits),
        pltpu.HBM((width, width), BF16),
        [*blocks, *halves],
        1 << 28,
        scratch=[pltpu.SemaphoreType.DMA((2 * nz,))],
        out_specs=HBM,
    )
    return call(
        finish_kernel,
        pltpu.HBM((2 * owners, 4 * width), BF16),
        [pltpu.with_memory_space_constraint(weight, pltpu.HBM), received, ln_gain, ln_bias],
        1 << 31,
        scratch=[
            pltpu.VMEM((width, width), BF16),
            pltpu.VMEM((lines, width), F32),
            pltpu.VMEM((2 * owners, 4 * width), BF16),
            pltpu.SemaphoreType.DMA((16,)),
        ],
        in_specs=[HBM, VMEM, VMEM, VMEM],
        out_specs=HBM,
        limit=24,
    )


def solution(mesh):
    placed = (
        P(("dp", "seq"), None),
        P(("dp", "seq"), None),
        P(("dp", "seq"), None),
        P(("dp", "seq"), None),
        P(None, "dp"),
        P(),
        P(),
    )
    return jax.shard_map(step, mesh=mesh, in_specs=placed, out_specs=P(("dp", "seq"), None), check_vma=False)
```

```python
import functools

import jax
import jax.numpy as jnp
from jax import lax
from jax.experimental import pallas as pl
from jax.experimental.pallas import tpu as pltpu
from jax.sharding import PartitionSpec as P

HEADS = 16
IMGS = 4
DEAD = -1000
VMEM = pl.BlockSpec(memory_space=pltpu.VMEM)
SMEM = pl.BlockSpec(memory_space=pltpu.SMEM)
HBM = pl.BlockSpec(memory_space=pltpu.HBM)
F32 = jnp.float32
BF16 = jnp.bfloat16


def iota(shape, dim):
    return lax.broadcasted_iota(jnp.int32, shape, dim)


def pick(hits, values):
    return lax.dot_general(
        jnp.where(hits, 1.0, 0.0).astype(BF16), values, (((1,), (0,)), ((), ())), preferred_element_type=F32
    )


def call(kernel, out_shape, operands, flops, scratch=(), smem=0, limit=8, out_specs=VMEM, in_specs=None):
    return pl.pallas_call(
        kernel,
        out_shape=out_shape,
        in_specs=in_specs or [SMEM] * smem + [VMEM] * (len(operands) - smem),
        out_specs=out_specs,
        scratch_shapes=list(scratch),
        compiler_params=pltpu.CompilerParams(vmem_limit_bytes=limit * 1024 * 1024),
        cost_estimate=pl.CostEstimate(flops=flops, bytes_accessed=1 << 20, transcendentals=0),
    )(*operands)


def image_ends(counts_ref):
    ends, end = [], 0
    for image in range(IMGS):
        end = end + counts_ref[0, image]
        ends.append(end)
    return ends


def row_slots(ends, owner_ref, rows):
    groups = owner_ref.shape[1]
    lane, sub = iota((1, rows), 1), iota((rows, 1), 0)
    owners = jnp.broadcast_to(owner_ref[...], (8, groups)).astype(F32).astype(BF16)
    spread = jnp.where((iota((1, rows), 1) >> 2) == iota((groups, 1), 0), 1.0, 0.0).astype(BF16)
    owner_row = jnp.dot(owners, spread, preferred_element_type=F32)[0:1, :]
    owner_col = jnp.sum(jnp.where(sub == lane, owner_row, 0.0), axis=1, keepdims=True)
    first = lane - (lane & 3)
    earlier = (owner_col == owner_row) & (sub < first) & ((sub & 3) == 0) & (sub < ends[-1])
    slot = jnp.sum(jnp.where(earlier, 1.0, 0.0), axis=0, keepdims=True)
    return owner_row.astype(jnp.int32), slot, first < ends[-1], lane & 3


def front_kernel(
    counts_in, owner_in, packed_in, patch_in, send_out,
    counts_ref, owner_ref, packed_ref, patch_ref, context_ref, send_ref, done, left
):
    rows, width = patch_ref.shape
    head_size = width // HEADS
    pairs = ((counts_in, counts_ref), (owner_in, owner_ref), (patch_in, patch_ref), (packed_in, packed_ref))
    fetches = [pltpu.make_async_copy(src, dst, done.at[i]) for i, (src, dst) in enumerate(pairs)]
    for fetch in fetches:
        fetch.start()
    context_ref[...] = jnp.zeros_like(context_ref)
    for fetch in fetches[:3]:
        fetch.wait()
    ends = image_ends(counts_ref)
    owner_row, slot, live, part = row_slots(ends, owner_ref, rows)
    key = jnp.where(live, owner_row * 8 + slot.astype(jnp.int32) * 4 + part, DEAD)
    lines = send_ref.shape[0]
    hits = key == iota((lines, 1), 0)
    held = jnp.sum(jnp.where(hits, 1.0, 0.0), axis=1, keepdims=True)
    marker = jnp.where(held == 0.0, 64.0, 0.0)
    send_ref[:, :width] = (pick(hits, patch_ref[...]) + marker).astype(BF16)
    leaves = [pltpu.make_async_copy(send_ref.at[:, :width], send_out.at[:, :width], left.at[2])]
    leaves[0].start()
    fetches[3].wait()
    lane, sub = iota((1, rows), 1), iota((rows, 1), 0)
    segment_row = sum((lane >= end).astype(jnp.int32) for end in ends)
    segment_col = sum((sub >= end).astype(jnp.int32) for end in ends)
    same_image = segment_col == segment_row
    for head in range(HEADS):
        low = head * head_size
        start = min(low // 128 * 128, width - 256)
        column = iota((1, 256), 1) + start
        mine = (column >= low) & (column < low + head_size)
        queries = packed_ref[:, start : start + 256]
        queries = jnp.where(mine, queries, jnp.zeros_like(queries))
        keys = packed_ref[:, width + start : width + start + 256]
        scores = lax.dot_general(
            queries, keys, (((1,), (1,)), ((), ())), preferred_element_type=F32
        ) * head_size ** (-0.5)
        scores = jnp.where(same_image, scores, -1e30)
        expo = jnp.exp(scores - jnp.max(scores, axis=1, keepdims=True))
        weights = (expo / jnp.sum(expo, axis=1, keepdims=True)).astype(BF16)
        values = packed_ref[:, 2 * width + start : 2 * width + start + 256]
        mixed = jnp.dot(weights, values, preferred_element_type=F32).astype(BF16)
        context_ref[:, start : start + 256] = jnp.where(mine, mixed, context_ref[:, start : start + 256])
    for i in range(2):
        place = slice(i * lines // 2, (i + 1) * lines // 2)
        wanted = iota((lines // 2, 1), 0) + i * lines // 2
        send_ref[place, width:] = pick(key == wanted, context_ref[...]).astype(BF16)
        leaves.append(pltpu.make_async_copy(send_ref.at[place, width:], send_out.at[place, width:], left.at[i]))
        leaves[-1].start()
    for leave in leaves:
        leave.wait()


def norm(hidden, gain, bias):
    gain, bias = gain[None, :], bias[None, :]
    inverse = 1.0 / hidden.shape[1]
    centered = hidden - jnp.sum(hidden, axis=1, keepdims=True) * inverse
    row_var = jnp.sum(centered * centered, axis=1, keepdims=True) * inverse
    return centered * lax.rsqrt(row_var + 1e-06) * gain + bias


def project(context, weight):
    return lax.dot_general(context, weight, (((1,), (1,)), ((), ())), preferred_element_type=F32)


def gather_kernel(nz, splits, *refs):
    blocks, halves, (weight_out, done) = refs[:nz], refs[nz : nz + len(splits)], refs[nz + len(splits) :]
    block_width = blocks[0].shape[0]
    me = lax.axis_index("dp")
    z, c = lax.shift_right_logical(me, 1), lax.bitwise_and(me, 1)
    pieces = [(j, c, blocks[j]) for j in range(nz)]
    for part, ref in zip(splits, halves):
        pieces += [(j, 1 - c, ref.at[i]) for i, j in enumerate(part)]
    leaves = []
    for i, (j, core, ref) in enumerate(pieces):
        owner = lax.rem(z + j * (1 - 2 * core) + nz, nz) * 2 + core
        place = pl.ds(pl.multiple_of(owner * block_width, 16), block_width)
        leaves.append(pltpu.make_async_copy(ref, weight_out.at[place, :], done.at[i]))
        leaves[i].start()
    for leave in leaves:
        leave.wait()


def finish_kernel(weight_in, received_ref, gain_ref, bias_ref, out_ref, weight_ref, hidden_ref, joined_ref, done):
    lines, width = hidden_ref.shape
    step = 256
    fetches = []
    for i in range(width // step):
        part = slice(i * step, (i + 1) * step)
        fetches.append(pltpu.make_async_copy(weight_in.at[part, :], weight_ref.at[part, :], done.at[i]))
        fetches[i].start()
    for i, fetch in enumerate(fetches):
        fetch.wait()
        part = slice(i * step, (i + 1) * step)
        patches = received_ref[:, part].astype(F32)
        hidden_ref[:, part] = patches + project(received_ref[:, width:], weight_ref[part, :])
    leaves = []
    chunk = min(128, lines)
    slots = chunk // 4
    row = iota((chunk, 1), 0)
    wanted = (row & (slots - 1)) * 4 + (row >> (slots.bit_length() - 1))
    hits = iota((1, chunk), 1) == wanted
    for i in range(lines // chunk):
        part = slice(i * chunk, (i + 1) * chunk)
        normed = norm(hidden_ref[part, :], gain_ref[...], bias_ref[...])
        normed = jnp.where(received_ref[part, :1].astype(F32) > 32.0, 0.0, normed).astype(BF16)
        joined = pick(hits, normed).astype(BF16)
        place = slice(i * slots, (i + 1) * slots)
        for k in range(4):
            joined_ref[place, k * width : (k + 1) * width] = joined[k * slots : (k + 1) * slots]
        leave = pltpu.make_async_copy(joined_ref.at[place, :], out_ref.at[place, :], done.at[8 + i])
        leave.start()
        leaves.append(leave)
    for leave in leaves:
        leave.wait()


def pack_kernel(*refs):
    for i, ref in enumerate(refs[:-1]):
        refs[-1][i] = ref[...]


def pack(blocks):
    shape = jax.ShapeDtypeStruct((len(blocks), *blocks[0].shape), blocks[0].dtype)
    return call(pack_kernel, shape, blocks, 1 << 20, limit=1)


def ring_gather(shard):
    n_dp = lax.axis_size("dp")
    nz = n_dp // 2
    up = [(2 * z + c, 2 * ((z + 1 - 2 * c) % nz) + c) for z in range(nz) for c in range(2)]
    down = [(there, here) for here, there in up]
    swap = [(d, d ^ 1) for d in range(n_dp)]
    blocks = [None] * nz
    blocks[0] = shard
    from_below, from_above = shard, shard
    for step in range(1, nz // 2 + 1):
        from_below = lax.ppermute(from_below, "dp", up)
        blocks[(-step) % nz] = from_below
        if step < nz - step:
            from_above = lax.ppermute(from_above, "dp", down)
            blocks[step] = from_above
    order = sorted(range(nz), key=lambda j: min(j, nz - j))
    splits = [s for s in (order[: nz // 2 + 1], order[nz // 2 + 1 :]) if s]
    halves = [lax.ppermute(pack([blocks[j] for j in part]), "dp", swap) for part in splits]
    return blocks, splits, halves


def step(patches, query_key_value, counts, owner_index, out_weight, ln_gain, ln_bias):
    rows, width = patches.shape
    owners = lax.axis_size("seq")
    nz = lax.axis_size("dp") // 2
    owner_lanes = owner_index.reshape(1, rows // 4)
    lines = 8 * owners

    blocks, splits, halves = ring_gather(out_weight.T)
    send = call(
        front_kernel,
        pltpu.HBM((lines, 2 * width), BF16),
        [pltpu.with_memory_space_constraint(x, pltpu.HBM) for x in (counts, owner_lanes, query_key_value, patches)],
        1 << 31,
        scratch=[
            pltpu.SMEM(counts.shape, jnp.int32),
            pltpu.VMEM(owner_lanes.shape, jnp.int32),
            pltpu.VMEM((rows, 3 * width), BF16),
            pltpu.VMEM((rows, width), BF16),
            pltpu.VMEM((rows, width), BF16),
            pltpu.VMEM((lines, 2 * width), BF16),
            pltpu.SemaphoreType.DMA((4,)),
            pltpu.SemaphoreType.DMA((3,)),
        ],
        in_specs=[HBM] * 4,
        out_specs=HBM,
        limit=16,
    )
    received = lax.all_to_all(send, "seq", split_axis=0, concat_axis=0, tiled=True)
    weight = call(
        functools.partial(gather_kernel, nz, splits),
        pltpu.HBM((width, width), BF16),
        [*blocks, *halves],
        1 << 28,
        scratch=[pltpu.SemaphoreType.DMA((2 * nz,))],
        out_specs=HBM,
    )
    return call(
        finish_kernel,
        pltpu.HBM((2 * owners, 4 * width), BF16),
        [pltpu.with_memory_space_constraint(weight, pltpu.HBM), received, ln_gain, ln_bias],
        1 << 31,
        scratch=[
            pltpu.VMEM((width, width), BF16),
            pltpu.VMEM((lines, width), F32),
            pltpu.VMEM((2 * owners, 4 * width), BF16),
            pltpu.SemaphoreType.DMA((16,)),
        ],
        in_specs=[HBM, VMEM, VMEM, VMEM],
        out_specs=HBM,
        limit=24,
    )


def solution(mesh):
    placed = (
        P(("dp", "seq"), None),
        P(("dp", "seq"), None),
        P(("dp", "seq"), None),
        P(("dp", "seq"), None),
        P(None, "dp"),
        P(),
        P(),
    )
    return jax.shard_map(step, mesh=mesh, in_specs=placed, out_specs=P(("dp", "seq"), None), check_vma=False)
```
